32 devices in a mesh: row: 8 (over y, x, core), col: 4 (over z).
Axes of the slice: x: 2, y: 2, z: 4, core: 2. Of those that a mesh axis runs over, the one named last changes fastest.
Arguments:
- hidden_in: bfloat16 [4096, 2048], P(('row', 'col')), may hold values from -6 to 6
- first_gain: float32 [2048], replicated, may hold values from 0.25 to 1.75
- query_weight: bfloat16 [2048, 4096], P(None, 'col'), may hold values from -0.125 to 0.125
- key_projection: bfloat16 [2048, 512], replicated, may hold values from -0.125 to 0.125
- value_projection: bfloat16 [2048, 512], replicated, may hold values from -0.125 to 0.125
- out_weight: bfloat16 [4096, 2048], P('col'), may hold values from -0.375 to 0.375
- query_gain: float32 [128], replicated, may hold values from 0.6 to 1.6, as said below
- key_gain: float32 [128], replicated, may hold values from 0.6 to 1.6, as said below
- second_gain: float32 [2048], replicated, may hold values from 0.25 to 1.75
- router_weight: bfloat16 [2048, 32], replicated, may hold values from -2 to 2
- gate_weight: bfloat16 [32, 2048, 768], P(('row', 'col')), may hold values from -0.125 to 0.125
- up_weight: bfloat16 [32, 2048, 768], P(('row', 'col')), may hold values from -0.125 to 0.125
- down_weight: bfloat16 [32, 768, 2048], P(('row', 'col')), may hold values from -0.21875 to 0.21875
- segments: int32 [8, 512], P('row'), may hold values from 0 to 2, never falling along the last dimension, each value on 1 to 480 neighbouring positions
- routes: int32 [4096, 8], P(('row', 'col')), may hold values from 0 to 31, all different within a row; in each aligned block of 128 rows (0 to 127, 128 to 255, ...) at most 36 rows name the same one
- cotangent: bfloat16 [4096, 2048], P(('row', 'col')), may hold values from -6 to 6
Outputs:
- block_out: bfloat16 [4096, 2048], P(('row', 'col'))
- input_grad: bfloat16 [4096, 2048], P(('row', 'col'))
- first_gain_grad: float32 [2048], replicated
- query_weight_grad: float32 [2048, 4096], P(None, 'col')
- key_weight_grad: float32 [2048, 512], replicated
- value_weight_grad: float32 [2048, 512], replicated
- out_weight_grad: float32 [4096, 2048], P('col')
- query_gain_grad: float32 [128], replicated
- key_gain_grad: float32 [128], replicated
- second_gain_grad: float32 [2048], replicated
- router_weight_grad: float32 [2048, 32], replicated
- gate_weight_grad: float32 [32, 2048, 768], P(('row', 'col'))
- up_weight_grad: float32 [32, 2048, 768], P(('row', 'col'))
- down_weight_grad: float32 [32, 768, 2048], P(('row', 'col'))
The draws below stay inside these ranges and needn't reach their ends.
Inputs may be any that keep to these rules, and one draw needn't show every extreme that they name: In the rows of one device (128 tokens, aligned blocks) no expert is named by more than 36 routes, a bound that some block reaches; a token's 8 routes are different experts. `segments`: in each token group the ids start at 0 and never fall; every sequence has 1 to 480 tokens and one has exactly 480. `query_gain`: positive gains. `key_gain`: positive gains.
All inputs are finite; a program needn't handle non-finite values.
Results may differ from the reference program's by a relative error of at most 0.023.
Values may be sent and summed in bfloat16 or wider, within the bound.
A program may use at most 256 MiB of HBM per device.

```python
import math
import jax
import jax.numpy as jnp
import numpy as np
from jax import lax

MODEL_DIM = 2048
QUERY_HEADS = 32
KEY_VALUE_HEADS = 4
HEAD_SIZE = 128
EXP_HID = 768
TOP = 8
TOK_DEV = 128
INDEX_TOKENS = 512
TOTAL_TOKENS = 4096
EXPERTS = 32
SEQ_MOST = 480
SEQS = 3
CAP = 36
N_ROW = 8
N_COL = 4


def draw_query_gain(key, part):
    subkey = jax.random.fold_in(key, 11)
    return jax.random.uniform(subkey, (HEAD_SIZE,), jnp.float32, 0.6, 1.6)


def draw_key_gain(key, part):
    subkey = jax.random.fold_in(key, 12)
    return jax.random.uniform(subkey, (HEAD_SIZE,), jnp.float32, 0.6, 1.6)


def draw_router_weight(key, part):
    subkey = jax.random.fold_in(key, 13)
    base = jnp.clip(jax.random.normal(subkey, (MODEL_DIM, EXPERTS), jnp.float32), -4.0, 4.0)
    return (base * (0.6 / math.sqrt(MODEL_DIM))).astype(jnp.bfloat16)


def shard_levels(key, dims, cuts, least, top_value):
    loudness, own = 1.0, jax.random.fold_in(key, 6)
    for dim, shards_of in cuts:
        heights = jnp.exp(jax.random.uniform(jax.random.fold_in(own, dim), (shards_of,), jnp.float32, least / len(cuts), top_value / len(cuts)))
        loudness = loudness * jnp.repeat(heights, dims[dim] // shards_of).reshape([-1 if axis == dim else 1 for axis in range(len(dims))])
    return loudness


def length_profile(amount, total, bound, slope):
    loads = [(1 << 20) // math.isqrt(rank ** slope) + 1 for rank in range(2, amount + 1)]
    spare, given = total - bound - (amount - 1), [1] * (amount - 1)
    while spare > 0:
        movable = [i for i in range(amount - 1) if given[i] < bound]
        mass, budget = sum([loads[i] for i in movable]), spare
        for i in movable:
            extra = min(bound - given[i], max(1, budget * loads[i] // mass), spare)
            given[i] = given[i] + extra
            spare = spare - extra
    return np.array([bound] + given)


def ragged_sizes(key, count, total, most, skew):
    if count == 2:
        one = jax.random.randint(key, (), max(1, total - most), min(most, total - 1) + 1)
        return jnp.stack([one, total - one])
    lengths = jnp.asarray(length_profile(count, total, most, skew), jnp.int32)
    twos = (count - 1) // 2
    source_of, sink = lengths[1:1 + 2 * twos:2], lengths[2:2 + 2 * twos:2]
    slack = jnp.minimum(source_of - 1, most - sink)
    shifted = jax.random.randint(jax.random.fold_in(key, 1), (twos,), 0, 1 << 20) % (slack + 1)
    lengths = lengths.at[1:1 + 2 * twos:2].set(source_of - shifted).at[2:2 + 2 * twos:2].set(sink + shifted)
    return lengths[jax.random.permutation(jax.random.fold_in(key, 2), count)]


def routed_block(own_key, own, number, rows, amount, top, most, lean):
    order = jax.random.permutation(own_key, amount)
    crowded, common = shares(amount, rows * top, most, lean, True), shares(amount, rows * top, most, lean, False)
    places = jnp.arange(amount)

    def named(lengths, rotation):
        used = int((lengths > 0).sum())
        fixed = max(1, used // 4)
        passed = fixed + (places - fixed + rotation * (used - fixed)) % max(1, amount - fixed)
        return jnp.zeros((amount,), jnp.int32).at[order[jnp.where(places < fixed, places, passed)]].set(jnp.asarray(lengths, jnp.int32))

    lengths = jnp.where(number % 4 == 0, named(crowded, number // 4), named(common, number - number // 4 - 1))
    mixed = jax.random.permutation(jax.random.fold_in(own, 3), amount)
    source_of, sink = mixed[0:amount // 2 * 2:2], mixed[1:amount // 2 * 2:2]
    room = jnp.minimum(lengths[source_of] - 1, most - lengths[sink]) // 2
    room = jnp.where((source_of == order[0]) | (sink == order[0]) | (lengths[sink] == 0), 0, jnp.maximum(room, 0))
    passed = jax.random.randint(jax.random.fold_in(own, 4), (amount // 2,), 0, 1 << 20) % (room + 1)
    lengths = lengths.at[source_of].add(-passed).at[sink].add(passed)
    items = jnp.searchsorted(jnp.cumsum(lengths), jnp.arange(rows * top), side="right").astype(jnp.int32)
    table = items.reshape(top, rows).T
    table = table[jax.random.permutation(jax.random.fold_in(own, 1), rows)]
    rotation = jax.random.randint(jax.random.fold_in(own, 2), (rows, 1), 0, top)
    return jnp.take_along_axis(table, (jnp.arange(top)[None, :] + rotation) % top, axis=1)


def shares(count, total, reach, skew, full):
    loads = [(1 << 20) // math.isqrt(grade ** skew) + 1 for grade in range(1, count + 1)]
    largest = reach if full else min(reach, max(-(-total // count), total * loads[0] // sum(loads)))
    least = 1 if total - largest >= count - 1 else 0
    holding, surplus = [largest] + [least] * (count - 1), total - largest - least * (count - 1)
    while surplus > 0:
        movable = [i for i in range(1, count) if holding[i] < largest] or [i for i in range(1, count) if holding[i] < reach]
        whole, left = sum([loads[i] for i in movable]), surplus
        for i in movable:
            more = min(reach - holding[i], max(1, left * loads[i] // whole), surplus)
            holding[i] = holding[i] + more
            surplus = surplus - more
    return np.array(holding)


def gaussian(own_key, dims, spread, limit, cuts=(), held_as=jnp.bfloat16):
    values = spread * jax.random.normal(own_key, dims, jnp.float32)
    if cuts:
        values = values * shard_levels(own_key, dims, cuts, -0.22, 0.18)
    return jnp.clip(values, -limit, limit).astype(held_as)


def setup_inputs(seed: int = 0) -> dict:
    key_of = jax.random.split(jax.random.key(seed), 17)
    hidden_in = gaussian(key_of[0], (TOTAL_TOKENS, MODEL_DIM), 1.0, 6.0, ((0, 32),))
    first_gain = jnp.clip(1.0 + 0.15 * jax.random.normal(key_of[1], (MODEL_DIM,), jnp.float32), 0.25, 1.75)
    query_weight = gaussian(key_of[2], (MODEL_DIM, QUERY_HEADS * HEAD_SIZE), MODEL_DIM ** -0.5, 0.125, ((1, 4),))
    key_projection = gaussian(key_of[3], (MODEL_DIM, KEY_VALUE_HEADS * HEAD_SIZE), MODEL_DIM ** -0.5, 0.125)
    value_projection = gaussian(key_of[4], (MODEL_DIM, KEY_VALUE_HEADS * HEAD_SIZE), MODEL_DIM ** -0.5, 0.125)
    out_weight = gaussian(key_of[5], (QUERY_HEADS * HEAD_SIZE, MODEL_DIM), (QUERY_HEADS * HEAD_SIZE // 16) ** -0.5, 0.375, ((0, 4),))
    query_gain = draw_query_gain(jax.random.fold_in(key_of[16], 71), 0)
    key_gain = draw_key_gain(jax.random.fold_in(key_of[16], 71), 0)
    second_gain = jnp.clip(1.0 + 0.15 * jax.random.normal(key_of[8], (MODEL_DIM,), jnp.float32), 0.25, 1.75)
    router_weight = draw_router_weight(jax.random.fold_in(key_of[16], 71), 0)
    gate_weight = gaussian(key_of[10], (EXPERTS, MODEL_DIM, EXP_HID), MODEL_DIM ** -0.5, 0.125, ((0, 32),))
    up_weight = gaussian(key_of[11], (EXPERTS, MODEL_DIM, EXP_HID), MODEL_DIM ** -0.5, 0.125, ((0, 32),))
    down_weight = gaussian(key_of[12], (EXPERTS, EXP_HID, MODEL_DIM), EXP_HID ** -0.5, 0.21875, ((0, 32),))
    segments = jax.vmap(lambda own: jnp.searchsorted(jnp.cumsum(ragged_sizes(own, SEQS, INDEX_TOKENS, SEQ_MOST, 1)), jnp.arange(INDEX_TOKENS), side="right"))(jax.random.split(key_of[13], N_ROW)).reshape((N_ROW, INDEX_TOKENS)).astype(jnp.int32)
    routes_keys = jax.random.split(jax.random.fold_in(key_of[14], 1), TOTAL_TOKENS // TOK_DEV)
    routes_turns = jax.random.permutation(jax.random.fold_in(key_of[14], 3), TOTAL_TOKENS // TOK_DEV)
    routes = jax.vmap(lambda own, number: routed_block(jax.random.fold_in(key_of[14], 2), own, number, TOK_DEV, EXPERTS, TOP, CAP, 1))(routes_keys, routes_turns).reshape((TOTAL_TOKENS, TOP))
    cotangent = gaussian(key_of[15], (TOTAL_TOKENS, MODEL_DIM), 1.0, 6.0, ((0, 32),))
    return dict(hidden_in=hidden_in, first_gain=first_gain, query_weight=query_weight, key_projection=key_projection, value_projection=value_projection, out_weight=out_weight, query_gain=query_gain, key_gain=key_gain, second_gain=second_gain, router_weight=router_weight, gate_weight=gate_weight, up_weight=up_weight, down_weight=down_weight, segments=segments, routes=routes, cotangent=cotangent)


@jax.custom_vjp
def low(v):
    return lax.optimization_barrier(v.astype(jnp.bfloat16)).astype(jnp.float32)

@jax.custom_vjp
def low_back(v):
    return v

def low_keep(v):
    return (low(v), None)

def low_pass(kept, grad):
    return (grad,)

def back_keep(v):
    return (v, None)

def back_low(kept, grad):
    return (low(grad),)
low.defvjp(low_keep, low_pass)
low_back.defvjp(back_keep, back_low)
EPSILON = 1e-06
THETA = 1000000.0
PRECISE = lax.Precision.HIGHEST
NEGATIVE = -1e+30

def matrix_product(left_side, right_side):
    return jnp.dot(left_side, right_side, precision=PRECISE, preferred_element_type=jnp.float32)

def norm_rows(values, gain):
    return values * lax.rsqrt(lax.optimization_barrier(jnp.mean(values * values, axis=-1, keepdims=True)) + EPSILON) * gain

def positions(segment_row):
    index = jnp.arange(segment_row.shape[0], dtype=jnp.int32)
    begins = jnp.concatenate([jnp.ones((1,), dtype=jnp.bool_), segment_row[1:] != segment_row[:-1]])
    first = lax.cummax(jnp.where(begins, index, 0).astype(jnp.int32), axis=0)
    return index - first

def rotate(values, places):
    half_width = HEAD_SIZE // 2
    freqs = THETA ** (-2.0 * jnp.arange(half_width, dtype=jnp.float32) / HEAD_SIZE)
    angles = places.astype(jnp.float32)[:, None] * freqs[None, :]
    cosine = jnp.cos(angles)[:, None, :]
    sine = jnp.sin(angles)[:, None, :]
    lower = values[..., :half_width]
    upper = values[..., half_width:]
    return jnp.concatenate([lower * cosine - upper * sine, upper * cosine + lower * sine], axis=-1)

def attend_query_group(pieces):
    query_rotated, key_rotated, value_lowered, segment_row = pieces
    index = jnp.arange(INDEX_TOKENS, dtype=jnp.int32)
    allowed = (index[None, :] <= index[:, None]) & (segment_row[None, :] == segment_row[:, None])
    grouped_heads = query_rotated.reshape(INDEX_TOKENS, KEY_VALUE_HEADS, QUERY_HEADS // KEY_VALUE_HEADS, HEAD_SIZE).transpose(1, 0, 2, 3)

    def per_head(parts):
        query_part, key_part, value_part = parts
        scores = jnp.einsum('qhd,kd->hqk', query_part, key_part, precision=PRECISE) * HEAD_SIZE ** (-0.5)
        scores = jnp.where(allowed[None], low_back(scores), NEGATIVE)
        top_score = lax.optimization_barrier(jnp.max(scores, axis=-1, keepdims=True))
        raised = jnp.exp(scores - top_score)
        softmax_out = low(raised / lax.optimization_barrier(jnp.sum(raised, axis=-1, keepdims=True)))
        return jnp.einsum('hqk,kd->qhd', softmax_out, value_part, precision=PRECISE)
    heads_out = lax.map(per_head, (grouped_heads, key_rotated.transpose(1, 0, 2), value_lowered.transpose(1, 0, 2)))
    return heads_out.transpose(1, 0, 2, 3).reshape(INDEX_TOKENS, QUERY_HEADS * HEAD_SIZE)

def expert_mix(mixer_in, route_weights, routes, gate_weight, up_weight, down_weight):
    flat_routes = routes.reshape(-1)
    flat_weights = route_weights.reshape(-1)
    room = N_ROW * N_COL * CAP

    def contribute(expert, gate_one, up_one, down_one):
        matches = flat_routes == expert
        picked = jnp.nonzero(matches, size=room, fill_value=0)[0].astype(jnp.int32)
        live = (jnp.arange(room, dtype=jnp.int32) < jnp.sum(matches.astype(jnp.int32))).astype(jnp.float32)
        token_index = picked // TOP
        rows_in = low_back(mixer_in[token_index])
        gate_value = low_back(matrix_product(rows_in, gate_one))
        up_value = low_back(matrix_product(rows_in, up_one))
        activated = low(gate_value * jax.nn.sigmoid(gate_value) * up_value)
        expert_rows = low_back(low(matrix_product(activated, down_one)))
        scaled = expert_rows * (flat_weights[picked] * live)[:, None]
        return jnp.zeros((TOTAL_TOKENS, MODEL_DIM), jnp.float32).at[token_index].add(scaled)

    def step(running, item):
        expert, gate_one, up_one, down_one = item
        return (running + jax.checkpoint(contribute)(expert, gate_one, up_one, down_one), None)
    experts_index = jnp.arange(EXPERTS, dtype=jnp.int32)
    mixed, unused = lax.scan(step, jnp.zeros((TOTAL_TOKENS, MODEL_DIM), jnp.float32), (experts_index, gate_weight, up_weight, down_weight))
    return mixed

def forward(hidden_in, first_gain, query_weight, key_projection, value_projection, out_weight, query_gain, key_gain, second_gain, router_weight, gate_weight, up_weight, down_weight, segments, routes):
    normed_input = low(norm_rows(hidden_in, first_gain))
    places = jax.vmap(positions)(segments).reshape(TOTAL_TOKENS)
    query_raw = low_back(matrix_product(normed_input, query_weight)).reshape(TOTAL_TOKENS, QUERY_HEADS, HEAD_SIZE)
    key_unrotated = low_back(matrix_product(normed_input, key_projection)).reshape(TOTAL_TOKENS, KEY_VALUE_HEADS, HEAD_SIZE)
    value_lowered = low(low_back(matrix_product(normed_input, value_projection))).reshape(TOTAL_TOKENS, KEY_VALUE_HEADS, HEAD_SIZE)
    query_rotated = low(rotate(norm_rows(query_raw, query_gain), places))
    key_rotated = low(rotate(norm_rows(key_unrotated, key_gain), places))
    attention_output = lax.map(jax.checkpoint(attend_query_group), (query_rotated.reshape(N_ROW, INDEX_TOKENS, QUERY_HEADS, HEAD_SIZE), key_rotated.reshape(N_ROW, INDEX_TOKENS, KEY_VALUE_HEADS, HEAD_SIZE), value_lowered.reshape(N_ROW, INDEX_TOKENS, KEY_VALUE_HEADS, HEAD_SIZE), segments))
    attention_output = low_back(low(attention_output.reshape(TOTAL_TOKENS, QUERY_HEADS * HEAD_SIZE)))
    branch = low_back(matrix_product(attention_output, out_weight))
    resid = hidden_in + branch
    mixer_in = low(norm_rows(resid, second_gain))
    logits = low_back(matrix_product(mixer_in, router_weight))
    chosen = jnp.take_along_axis(logits, routes, axis=1)
    top_logit = lax.optimization_barrier(jnp.max(chosen, axis=1, keepdims=True))
    raised = jnp.exp(chosen - top_logit)
    route_weights = raised / lax.optimization_barrier(jnp.sum(raised, axis=1, keepdims=True))
    mixed = expert_mix(mixer_in, route_weights, routes, gate_weight, up_weight, down_weight)
    return resid + mixed

def reference(hidden_in, first_gain, query_weight, key_projection, value_projection, out_weight, query_gain, key_gain, second_gain, router_weight, gate_weight, up_weight, down_weight, segments, routes, cotangent):
    params = (hidden_in.astype(jnp.float32), first_gain.astype(jnp.float32), query_weight.astype(jnp.float32), key_projection.astype(jnp.float32), value_projection.astype(jnp.float32), out_weight.astype(jnp.float32), query_gain.astype(jnp.float32), key_gain.astype(jnp.float32), second_gain.astype(jnp.float32), router_weight.astype(jnp.float32), gate_weight.astype(jnp.float32), up_weight.astype(jnp.float32), down_weight.astype(jnp.float32))

    def run(*values):
        return forward(*values, segments, routes)
    result, pull = jax.vjp(run, *params)
    grads = pull(cotangent.astype(jnp.float32))
    return (result.astype(jnp.bfloat16), grads[0].astype(jnp.bfloat16), grads[1], grads[2], grads[3], grads[4], grads[5], grads[6], grads[7], grads[8], grads[9], grads[10], grads[11], grads[12])
```

```python
import functools

import jax
import jax.numpy as jnp
from jax import lax
from jax.experimental import pallas as pl
from jax.experimental.pallas import tpu as pltpu
from jax.sharding import PartitionSpec as P

QUERY_HEADS = 32
KEY_VALUE_HEADS = 4
HEAD_SIZE = 128
TOP = 8

EPSILON = 1e-06
THETA = 1000000.0
NEGATIVE = -1e30
MESH_ID = pl.DeviceIdType.MESH
BF = jnp.bfloat16
F32 = jnp.float32


def exchange_kernel(plan, *refs):
    count = len(plan)
    ins, outs = refs[:count], refs[count : 2 * count]
    local_sems, send_sems, recv_sems = refs[2 * count :]
    axes = {axis: size for axis, size, _ in plan}
    barrier = pltpu.get_barrier_semaphore()
    for axis, size in axes.items():
        me = lax.axis_index(axis)
        for step in range(1, size):
            pl.semaphore_signal(
                barrier, inc=1, device_id={axis: lax.rem(me + step, size)}, device_id_type=MESH_ID
            )
    pl.semaphore_wait(barrier, sum(size - 1 for size in axes.values()))
    remote = []
    local = []
    slot = 0
    for item, (axis, size, mode) in enumerate(plan):
        me = lax.axis_index(axis)
        for step in range(1, size):
            to = lax.rem(me + step, size)
            copy = pltpu.make_async_remote_copy(
                src_ref=ins[item] if mode == "gather" else ins[item].at[to],
                dst_ref=outs[item].at[me],
                send_sem=send_sems.at[slot],
                recv_sem=recv_sems.at[slot],
                device_id={axis: to},
                device_id_type=MESH_ID,
            )
            copy.start()
            remote.append(copy)
            slot += 1
        copy = pltpu.make_async_copy(
            ins[item] if mode == "gather" else ins[item].at[me], outs[item].at[me], local_sems.at[item]
        )
        copy.start()
        local.append(copy)
    for copy in local:
        copy.wait()
    for copy in remote:
        copy.wait()


def exchange(number, name, *items):
    plan = [(axis, size, mode) for _, axis, size, mode in items]
    slots = sum(size - 1 for _, size, _ in plan)
    shapes = []
    for array, _, size, mode in items:
        shape = (size,) + array.shape if mode == "gather" else array.shape
        shapes.append(jax.ShapeDtypeStruct(shape, array.dtype))
    return pl.pallas_call(
        functools.partial(exchange_kernel, plan),
        out_shape=tuple(shapes),
        in_specs=[pl.BlockSpec(memory_space=pl.ANY)] * len(items),
        out_specs=tuple([pl.BlockSpec(memory_space=pl.ANY)] * len(items)),
        scratch_shapes=[
            pltpu.SemaphoreType.DMA((len(items),)),
            pltpu.SemaphoreType.DMA((slots,)),
            pltpu.SemaphoreType.DMA((slots,)),
        ],
        compiler_params=pltpu.CompilerParams(collective_id=number, has_side_effects=True),
        name=name,
    )(*[item[0] for item in items])


def bits_of(size):
    return [bit for bit in range(size.bit_length() - 1)]


def add_rows(target, begin, source, rows, step=64):
    step = min(step, rows)

    def body(i, carry):
        at = pl.ds(pl.multiple_of(begin + i * step, step), step)
        source_at = pl.ds(pl.multiple_of(i * step, step), step)
        target[at, :] = (target[at, :].astype(F32) + source[source_at, :].astype(F32)).astype(BF)
        return carry

    lax.fori_loop(0, rows // step, body, 0)


def tail_kernel(
    n_row,
    n_col,
    orders,
    parts_ref,
    out_in,
    query_in,
    side_in,
    gains_ref,
    parts_out,
    out_out,
    query_out,
    side_out,
    gains_out,
    out_ref,
    query_ref,
    side_ref,
    out_buf,
    query_buf,
    side_buf,
    plane_buf,
    gains_plane,
    gains_buf,
    local_sem,
    part_send,
    part_recv,
    send_sems,
    recv_sems,
    plane_send,
    plane_recv,
    gains_send,
    gains_recv,
):
    row, col = lax.axis_index("row"), lax.axis_index("col")
    stages = len(orders[0])
    sums = (out_ref, query_ref, side_ref)
    buffers = (out_buf, query_buf, side_buf)
    results = (out_out, query_out, side_out)
    count = len(sums)
    side = count - 1
    loads = [
        pltpu.make_async_copy(source, target, local_sem.at[1 + i])
        for i, (source, target) in enumerate(zip((out_in, query_in, side_in), sums))
    ]
    for copy in loads:
        copy.start()
    barrier = pltpu.get_barrier_semaphore()
    for step in range(1, n_col):
        pl.semaphore_signal(
            barrier, inc=1, device_id={"col": lax.rem(col + step, n_col)}, device_id_type=MESH_ID
        )
    mine = {bit: lax.rem(row // (1 << bit), 2) for bit in orders[0]}
    peer = {bit: row + (1 - 2 * mine[bit]) * (1 << bit) for bit in orders[0]}
    for bit in orders[0]:
        pl.semaphore_signal(barrier, inc=1, device_id={"row": peer[bit]}, device_id_type=MESH_ID)
    pl.semaphore_wait(barrier, n_col - 1 + stages)

    part_copies = []
    for step in range(1, n_col):
        to = lax.rem(col + step, n_col)
        copy = pltpu.make_async_remote_copy(
            src_ref=parts_ref.at[to],
            dst_ref=parts_out.at[col],
            send_sem=part_send.at[step - 1],
            recv_sem=part_recv.at[step - 1],
            device_id={"col": to},
            device_id_type=MESH_ID,
        )
        copy.start()
        part_copies.append(copy)
    own = pltpu.make_async_copy(parts_ref.at[col], parts_out.at[col], local_sem.at[0])
    own.start()
    gain_copies = []
    for step in range(1, n_col):
        copy = pltpu.make_async_remote_copy(
            src_ref=gains_ref,
            dst_ref=gains_plane.at[col],
            send_sem=gains_send.at[step - 1],
            recv_sem=gains_recv.at[step - 1],
            device_id={"col": lax.rem(col + step, n_col)},
            device_id_type=MESH_ID,
        )
        copy.start()
        gain_copies.append(copy)
    gains_plane[col] = gains_ref[...]
    for copy in loads:
        copy.wait()

    low = [[stream * (array.shape[0] // 2) for stream in range(2)] for array in sums]
    length = [array.shape[0] // 4 for array in sums]

    def send_half(which, stream, stage):
        bit = orders[stream][stage]
        rows = length[which]
        half = sums[which].shape[0] // 2
        away = low[which][stream] + (1 - mine[bit]) * rows
        low[which][stream] = low[which][stream] + mine[bit] * rows
        place = stream * half + (half - 2 * rows)
        copy = pltpu.make_async_remote_copy(
            src_ref=sums[which].at[pl.ds(pl.multiple_of(away, rows), rows)],
            dst_ref=buffers[which].at[pl.ds(place, rows)],
            send_sem=send_sems.at[0, stage, stream, which],
            recv_sem=recv_sems.at[0, stage, stream, which],
            device_id={"row": peer[bit]},
            device_id_type=MESH_ID,
        )
        copy.start()
        return place, copy

    pending = {
        (which, stream): send_half(which, stream, 0) for which in reversed(range(count)) for stream in range(2)
    }
    for stage in range(stages):
        for which in reversed(range(count)):
            rows = length[which]
            if stage + 1 < stages:
                length[which] = rows // 2
            for stream in range(2):
                place, copy = pending[which, stream]
                copy.wait()
                add_rows(sums[which], low[which][stream], buffers[which].at[pl.ds(place, rows)], rows)
                if stage + 1 < stages:
                    pending[which, stream] = send_half(which, stream, stage + 1)

    def send_back(which, stage):
        array = results[which]
        rows = length[which]
        copies = []
        for stream in range(2):
            bit = orders[stream][stage]
            at = pl.ds(pl.multiple_of(low[which][stream], rows), rows)
            copy = pltpu.make_async_remote_copy(
                src_ref=array.at[at],
                dst_ref=array.at[at],
                send_sem=send_sems.at[1, stage, stream, which],
                recv_sem=recv_sems.at[1, stage, stream, which],
                device_id={"row": peer[bit]},
                device_id_type=MESH_ID,
            )
            copy.start()
            copies.append(copy)
            low[which][stream] = low[which][stream] - mine[bit] * rows
        length[which] = rows * 2
        return copies

    plane_copies = []
    rows = length[side]
    for stream in range(2):
        at = pl.ds(pl.multiple_of(low[side][stream], rows), rows)
        for step in range(1, n_col):
            copy = pltpu.make_async_remote_copy(
                src_ref=side_ref.at[at],
                dst_ref=plane_buf.at[col, stream],
                send_sem=plane_send.at[stream, step - 1],
                recv_sem=plane_recv.at[stream, step - 1],
                device_id={"col": lax.rem(col + step, n_col)},
                device_id_type=MESH_ID,
            )
            copy.start()
            plane_copies.append(copy)
        plane_buf[col, stream] = side_ref[at, :]
    pending = {}
    for which in range(side):
        for stream in range(2):
            at = pl.ds(pl.multiple_of(low[which][stream], length[which]), length[which])
            results[which][at, :] = sums[which][at, :]
        pending[which] = send_back(which, stages - 1)

    for copy in gain_copies:
        copy.wait()
    total = gains_plane[0]
    for plane in range(1, n_col):
        total = total + gains_plane[plane]
    for stage, bit in enumerate(orders[0]):
        gains_buf[stage, 0] = total
        copy = pltpu.make_async_remote_copy(
            src_ref=gains_buf.at[stage, 0],
            dst_ref=gains_buf.at[stage, 1],
            send_sem=gains_send.at[n_col - 1 + stage],
            recv_sem=gains_recv.at[n_col - 1 + stage],
            device_id={"row": peer[bit]},
            device_id_type=MESH_ID,
        )
        copy.start()
        copy.wait()
        total = gains_buf[stage, 0] + gains_buf[stage, 1]
    gains_out[...] = total

    for copy in plane_copies:
        copy.wait()
    head = HEAD_SIZE
    planes_a_head = n_col // KEY_VALUE_HEADS
    width = KEY_VALUE_HEADS * head
    for stream in range(2):
        at = pl.ds(pl.multiple_of(low[side][stream], rows), rows)
        for kv in range(2):
            for key_head in range(KEY_VALUE_HEADS):
                columns = slice(kv * head, (kv + 1) * head)
                total = plane_buf[key_head * planes_a_head, stream, :, columns]
                for other in range(1, planes_a_head):
                    total = (
                        total.astype(F32)
                        + plane_buf[key_head * planes_a_head + other, stream, :, columns].astype(F32)
                    ).astype(BF)
                begin = kv * width + key_head * head
                side_out[at, begin : begin + head] = total
        total = plane_buf[0, stream, :, 2 * head :].astype(F32)
        for plane in range(1, n_col):
            total = total + plane_buf[plane, stream, :, 2 * head :].astype(F32)
        side_out[at, 2 * width :] = total.astype(BF)
    pending[side] = send_back(side, stages - 1)
    for stage in reversed(range(stages)):
        for which in range(count):
            for copy in pending[which]:
                copy.wait()
            if stage:
                pending[which] = send_back(which, stage - 1)
    own.wait()
    for copy in part_copies:
        copy.wait()


def tail(number, n_row, n_col, parts, out_part, query_part, side_part, gains):
    model_rows, side_width = side_part.shape
    bits = bits_of(n_row)
    orders = (bits, bits[:1] + bits[:0:-1])
    stages = len(bits)
    segment = model_rows // 2 // n_row
    result_width = 2 * KEY_VALUE_HEADS * HEAD_SIZE + side_width - 2 * HEAD_SIZE
    vmem = pl.BlockSpec(memory_space=pltpu.VMEM)
    anywhere = pl.BlockSpec(memory_space=pl.ANY)
    summed = (out_part, query_part, side_part)
    return pl.pallas_call(
        functools.partial(tail_kernel, n_row, n_col, orders),
        out_shape=(
            jax.ShapeDtypeStruct(parts.shape, BF),
            jax.ShapeDtypeStruct(out_part.shape, BF),
            jax.ShapeDtypeStruct(query_part.shape, BF),
            jax.ShapeDtypeStruct((model_rows, result_width), BF),
            jax.ShapeDtypeStruct(gains.shape, F32),
        ),
        in_specs=[anywhere] * 4 + [vmem],
        out_specs=(anywhere, vmem, vmem, vmem, vmem),
        scratch_shapes=[pltpu.VMEM(array.shape, BF) for array in summed]
        + [pltpu.VMEM(array.shape, BF) for array in summed]
        + [
            pltpu.VMEM((n_col, 2, segment, side_width), BF),
            pltpu.VMEM((n_col,) + gains.shape, F32),
            pltpu.VMEM((stages, 2) + gains.shape, F32),
            pltpu.SemaphoreType.DMA((4,)),
            pltpu.SemaphoreType.DMA((n_col - 1,)),
            pltpu.SemaphoreType.DMA((n_col - 1,)),
            pltpu.SemaphoreType.DMA((2, stages, 2, 3)),
            pltpu.SemaphoreType.DMA((2, stages, 2, 3)),
            pltpu.SemaphoreType.DMA((2, n_col - 1)),
            pltpu.SemaphoreType.DMA((2, n_col - 1)),
            pltpu.SemaphoreType.DMA((n_col - 1 + stages,)),
            pltpu.SemaphoreType.DMA((n_col - 1 + stages,)),
        ],
        compiler_params=pltpu.CompilerParams(collective_id=number, has_side_effects=True),
        name="tail",
    )(parts, *summed, gains)


def norm_rows(values, gain):
    return values * lax.rsqrt(jnp.mean(values * values, axis=-1, keepdims=True) + EPSILON) * gain


def rope_tables(segment_row):
    tokens = segment_row.shape[0]
    index = jnp.arange(tokens, dtype=jnp.int32)
    first = jnp.sum((segment_row[None, :] < segment_row[:, None]).astype(jnp.int32), axis=1)
    half_width = HEAD_SIZE // 2
    freqs = THETA ** (-2.0 * jnp.arange(half_width, dtype=F32) / HEAD_SIZE)
    angles = (index - first).astype(F32)[:, None] * freqs[None, :]
    return (jnp.cos(angles)[:, None, :], jnp.sin(angles)[:, None, :])


def head_prep(raw, gain, cosine, sine):
    normed_input = norm_rows(raw, gain)
    half_width = HEAD_SIZE // 2
    lower = normed_input[..., :half_width]
    upper = normed_input[..., half_width:]
    return jnp.concatenate([lower * cosine - upper * sine, upper * cosine + lower * sine], axis=-1)


def route_softmax(chosen):
    top_logit = jnp.max(chosen, axis=1, keepdims=True)
    raised = jnp.exp(chosen - top_logit)
    return raised / jnp.sum(raised, axis=1, keepdims=True)


def allowed_block(segment_row, row_begin, row_end):
    query_index = jnp.arange(row_begin, row_end, dtype=jnp.int32)
    key_index = jnp.arange(0, row_end, dtype=jnp.int32)
    causal = key_index[None, :] <= query_index[:, None]
    same_seq = segment_row[None, :row_end] == segment_row[row_begin:row_end, None]
    return causal & same_seq


def dot(left, right, left_dim, right_dim):
    return lax.dot_general(
        left, right, (((left_dim,), (right_dim,)), ((), ())), preferred_element_type=F32
    )


def col_gather(block, n_col):
    col = lax.axis_index("col")
    rows = block.shape[0]
    whole = jnp.zeros((n_col * rows,) + block.shape[1:], block.dtype)
    whole = lax.dynamic_update_slice_in_dim(whole, block, col * rows, 0)
    for step in range(1, n_col):
        got = lax.ppermute(block, "col", [(i, (i + step) % n_col) for i in range(n_col)])
        whole = lax.dynamic_update_slice_in_dim(whole, got, (col - step) % n_col * rows, 0)
    return whole


def col_scatter(whole, n_col):
    col = lax.axis_index("col")
    rows = whole.shape[0] // n_col
    total = lax.dynamic_slice_in_dim(whole, col * rows, rows, 0).astype(F32)
    for step in range(1, n_col):
        sent = lax.dynamic_slice_in_dim(whole, (col + step) % n_col * rows, rows, 0)
        got = lax.ppermute(sent, "col", [(i, (i + step) % n_col) for i in range(n_col)])
        total = total + got.astype(F32)
    return total


def shards(
    n_row,
    n_col,
    hidden_in,
    first_gain,
    query_weight,
    key_projection,
    value_projection,
    out_weight,
    query_gain,
    key_gain,
    second_gain,
    router_weight,
    gate_weight,
    up_weight,
    down_weight,
    segments,
    routes,
    cotangent,
):
    tok_rows, model_width = hidden_in.shape
    expert_count = router_weight.shape[1]
    group_rows = tok_rows * n_col
    col = lax.axis_index("col")
    resid_in = hidden_in.astype(F32)
    normed_low = norm_rows(resid_in, first_gain).astype(BF)
    routes_wide = jnp.broadcast_to(routes[:, :, None], (tok_rows, TOP, 16)).reshape(tok_rows, TOP * 16)
    gathered, routes_got = exchange(
        0,
        "gather_normed",
        (normed_low, "col", n_col, "gather"),
        (routes_wide.astype(BF), "col", n_col, "gather"),
    )
    gathered = gathered.reshape(group_rows, model_width)
    group_routes = routes_got.reshape(group_rows, TOP, 16)[:, :, 0].astype(jnp.int32)

    capacity = max(2, tok_rows * TOP * 9 // (expert_count * 8)) * n_col
    capacity = -(-capacity // 16) * 16
    plane_expert = jnp.arange(n_row, dtype=jnp.int32) * n_col + col
    named = jnp.any(group_routes[None, :, :] == plane_expert[:, None, None], axis=2)
    index = jnp.arange(group_rows, dtype=jnp.int32)
    earlier = (index[:, None] < index[None, :]).astype(BF)
    rank = jnp.dot(named.astype(BF), earlier, preferred_element_type=F32).astype(jnp.int32)
    slot = jnp.arange(capacity, dtype=jnp.int32)
    select = (named[:, None, :] & (rank[:, None, :] == slot[None, :, None])).astype(BF)
    select = select.reshape(n_row * capacity, group_rows)

    cot_parts = col_gather(lax.optimization_barrier((cotangent, gathered))[0], n_col)

    segment_row = segments[0]
    cosine, sine = rope_tables(segment_row)
    heads_here = query_weight.shape[1] // HEAD_SIZE
    group_heads = QUERY_HEADS // KEY_VALUE_HEADS
    kv_start = col * heads_here // group_heads * HEAD_SIZE
    key_columns = lax.dynamic_slice_in_dim(key_projection, kv_start, HEAD_SIZE, 1)
    value_columns = lax.dynamic_slice_in_dim(value_projection, kv_start, HEAD_SIZE, 1)
    query_raw = jnp.dot(gathered, query_weight, preferred_element_type=F32).reshape(
        group_rows, heads_here, HEAD_SIZE
    )
    key_full = jnp.dot(gathered, key_columns, preferred_element_type=F32)
    value_full = jnp.dot(gathered, value_columns, preferred_element_type=F32)

    def prep_heads(raw, gain):
        return head_prep(raw, gain, cosine, sine)

    query_rotated, query_pull = jax.vjp(prep_heads, query_raw, query_gain)
    key_rotated, key_pull = jax.vjp(prep_heads, key_full[:, None, :], key_gain)
    query_low = query_rotated.astype(BF)
    key_low = key_rotated[:, 0, :].astype(BF)
    value_lowered = value_full.astype(BF)
    block_rows = max(min(512, group_rows), group_rows // 8)
    score_scale = HEAD_SIZE ** (-0.5)
    pieces_out = []
    log_totals = []
    for row_begin in range(0, group_rows, block_rows):
        row_end = row_begin + block_rows
        scores = (
            jnp.einsum(
                "qhd,kd->hqk", query_low[row_begin:row_end], key_low[:row_end], preferred_element_type=F32
            )
            * score_scale
        )
        scores = jnp.where(allowed_block(segment_row, row_begin, row_end)[None], scores, NEGATIVE)
        top_score = jnp.max(scores, axis=-1, keepdims=True)
        raised = jnp.exp(scores - top_score)
        row_total = jnp.sum(raised, axis=-1, keepdims=True)
        softmax_low = (raised / row_total).astype(BF)
        pieces_out.append(
            jnp.einsum("hqk,kd->qhd", softmax_low, value_lowered[:row_end], preferred_element_type=F32)
        )
        log_totals.append(top_score + jnp.log(row_total))
    attention_output = (
        jnp.concatenate(pieces_out, axis=0).reshape(group_rows, heads_here * HEAD_SIZE).astype(BF)
    )
    partial_branch = jnp.dot(attention_output, out_weight, preferred_element_type=F32).astype(BF)

    cot_out = jnp.dot(select, cot_parts, preferred_element_type=F32).astype(BF)
    branch_parts, cot_rows = exchange(
        1,
        "scatter_branch",
        (partial_branch.reshape(n_col, tok_rows, model_width), "col", n_col, "trade"),
        (cot_out.reshape(n_row, capacity, model_width), "row", n_row, "trade"),
    )
    resid = resid_in + jnp.sum(branch_parts.astype(F32), axis=0)
    mixer_in, second_pull = jax.vjp(norm_rows, resid, second_gain)
    (mixer_group,) = exchange(2, "gather_mixer", (mixer_in.astype(BF), "col", n_col, "gather"))
    mixer_group = mixer_group.reshape(group_rows, model_width)
    logits = jnp.dot(mixer_group, router_weight, preferred_element_type=F32)
    experts = jnp.arange(expert_count, dtype=jnp.int32)
    chosen_mask = jnp.any(group_routes[:, :, None] == experts[None, None, :], axis=1)
    masked = jnp.where(chosen_mask, logits, NEGATIVE)
    raised = jnp.where(chosen_mask, jnp.exp(masked - jnp.max(masked, axis=1, keepdims=True)), 0.0)
    weights_full = raised / jnp.sum(raised, axis=1, keepdims=True)
    column_here = (experts % n_col == col)[None, :]
    plane_weights = jnp.sum(
        jnp.where(column_here, weights_full, 0.0).reshape(group_rows, n_row, n_col), axis=2
    )
    select_f = select.reshape(n_row, capacity, group_rows)
    slot_weights = jnp.sum(
        jnp.where(select_f > 0, plane_weights.T[:, None, :], 0.0), axis=2
    )
    rows_out = jnp.dot(select, mixer_group, preferred_element_type=F32).astype(BF)
    rows_in, weights_in = exchange(
        3,
        "dispatch",
        (rows_out.reshape(n_row, capacity, model_width), "row", n_row, "trade"),
        (jnp.broadcast_to(slot_weights[:, None, :], (n_row, 8, capacity)), "row", n_row, "trade"),
    )
    slots = n_row * capacity
    rows_in = rows_in.reshape(slots, model_width)
    cot_rows = cot_rows.reshape(slots, model_width)
    row_weight = weights_in[:, 0, :].reshape(slots, 1)

    gate_value = dot(rows_in, gate_weight[0], 1, 0)
    up_value = dot(rows_in, up_weight[0], 1, 0)
    sigmoid_gate = jax.nn.sigmoid(gate_value)
    activated = gate_value * sigmoid_gate * up_value
    grad_act = dot(cot_rows, down_weight[0], 1, 1) * row_weight
    weighted_grad = jnp.sum(activated * grad_act, axis=1)
    grad_gate = (grad_act * up_value * sigmoid_gate * (1.0 + gate_value * (1.0 - sigmoid_gate))).astype(BF)
    grad_up = (grad_act * gate_value * sigmoid_gate).astype(BF)
    grad_rows = (dot(grad_gate, gate_weight[0], 1, 1) + dot(grad_up, up_weight[0], 1, 1)).astype(BF)
    grad_back, weighted_back = exchange(
        4,
        "return_grads",
        (grad_rows.reshape(n_row, capacity, model_width), "row", n_row, "trade"),
        (
            jnp.broadcast_to(weighted_grad.reshape(n_row, 1, capacity), (n_row, 8, capacity)),
            "row",
            n_row,
            "trade",
        ),
    )
    expert_rows = (dot(activated.astype(BF), down_weight[0], 1, 0) * row_weight).astype(BF)
    down_grad = dot((activated * row_weight).astype(BF), cot_rows, 0, 0)
    gate_grad = dot(rows_in, grad_gate, 0, 0)
    up_grad = dot(rows_in, grad_up, 0, 0)

    plane_grads = jnp.sum(jnp.where(select_f > 0, weighted_back[:, 0, :, None], 0.0), axis=1).T
    plane_total = jnp.sum(plane_grads, axis=1, keepdims=True)
    grad_logits = (
        jnp.where(column_here, jnp.repeat(plane_grads, n_col, axis=1), 0.0) - plane_total * weights_full
    ).astype(BF)
    router_grad = dot(mixer_group, grad_logits, 0, 0)
    grad_mixer_part = (
        dot(select, grad_back.reshape(slots, model_width), 0, 0) + dot(grad_logits, router_weight, 1, 1)
    ).astype(BF)
    grad_mixer_parts, expert_back = exchange(
        5,
        "scatter_grad_mixer",
        (grad_mixer_part.reshape(n_col, tok_rows, model_width), "col", n_col, "trade"),
        (expert_rows.reshape(n_row, capacity, model_width), "row", n_row, "trade"),
    )
    grad_mixer = jnp.sum(grad_mixer_parts.astype(F32), axis=0)
    grad_second, second_gain_grad = second_pull(grad_mixer)
    grad_resid = cotangent.astype(F32) + grad_second
    (grad_branch,) = exchange(6, "gather_grad_branch", (grad_resid.astype(BF), "col", n_col, "gather"))
    grad_branch = grad_branch.reshape(group_rows, model_width)
    mixed_part = dot(select, expert_back.reshape(slots, model_width), 0, 0).astype(BF)
    mixed = col_scatter(mixed_part, n_col)
    block_out = (resid + mixed).astype(BF)

    out_grad = jnp.einsum("gf,gd->fd", attention_output, grad_branch, preferred_element_type=F32)
    out_grad = out_grad.astype(BF)
    grad_attended = (
        jnp.einsum("gd,fd->gf", grad_branch, out_weight, preferred_element_type=F32)
        .astype(BF)
        .reshape(group_rows, heads_here, HEAD_SIZE)
    )
    query_grads = []
    key_grad = jnp.zeros((group_rows, HEAD_SIZE), F32)
    value_grad = jnp.zeros((group_rows, HEAD_SIZE), F32)
    for block_index, row_begin in enumerate(range(0, group_rows, block_rows)):
        row_end = row_begin + block_rows
        scores = (
            jnp.einsum(
                "qhd,kd->hqk", query_low[row_begin:row_end], key_low[:row_end], preferred_element_type=F32
            )
            * score_scale
        )
        scores = jnp.where(allowed_block(segment_row, row_begin, row_end)[None], scores, NEGATIVE)
        softmax_full = jnp.exp(scores - log_totals[block_index])
        softmax_low = softmax_full.astype(BF)
        grad_soft = jnp.einsum(
            "qhd,kd->hqk",
            grad_attended[row_begin:row_end],
            value_lowered[:row_end],
            preferred_element_type=F32,
        )
        grad_scores = (
            softmax_full * (grad_soft - jnp.sum(softmax_full * grad_soft, axis=-1, keepdims=True))
        ).astype(BF)
        query_grads.append(
            jnp.einsum("hqk,kd->qhd", grad_scores, key_low[:row_end], preferred_element_type=F32)
            * score_scale
        )
        key_grad = key_grad.at[:row_end].add(
            jnp.einsum("hqk,qhd->kd", grad_scores, query_low[row_begin:row_end], preferred_element_type=F32)
            * score_scale
        )
        value_grad = value_grad.at[:row_end].add(
            jnp.einsum(
                "hqk,qhd->kd", softmax_low, grad_attended[row_begin:row_end], preferred_element_type=F32
            )
        )
    grad_query_raw, query_gain_grad = query_pull(jnp.concatenate(query_grads, axis=0))
    grad_key_raw, key_gain_grad = key_pull(key_grad[:, None, :])
    query_grad_low = grad_query_raw.reshape(group_rows, heads_here * HEAD_SIZE).astype(BF)
    key_grad_low = grad_key_raw[:, 0, :].astype(BF)
    value_grad_low = value_grad.astype(BF)
    grad_normed_part = jnp.einsum("gf,df->gd", query_grad_low, query_weight, preferred_element_type=F32)
    grad_normed_part = grad_normed_part + jnp.einsum(
        "gf,df->gd", key_grad_low, key_columns, preferred_element_type=F32
    )
    grad_normed_part = grad_normed_part + jnp.einsum(
        "gf,df->gd", value_grad_low, value_columns, preferred_element_type=F32
    )
    query_grad = jnp.einsum("gd,gf->df", gathered, query_grad_low, preferred_element_type=F32)
    key_value_grad = dot(gathered, jnp.concatenate([key_grad_low, value_grad_low], axis=1), 0, 0)
    grad_normed_part = grad_normed_part.astype(BF)
    first_scale = lax.rsqrt(jnp.mean(resid_in * resid_in, axis=-1, keepdims=True) + EPSILON)
    first_gain_part = jnp.sum(grad_normed_part.astype(F32) * gathered.astype(F32), axis=0) / first_gain
    lane_pad = (0, model_width - HEAD_SIZE)
    gains = jnp.stack(
        [first_gain_part, second_gain_grad, jnp.pad(query_gain_grad, lane_pad), jnp.pad(key_gain_grad, lane_pad)]
    )
    gains = jnp.pad(gains, ((0, 4), (0, 0)))
    side = jnp.concatenate(
        [key_value_grad.astype(BF), jnp.pad(router_grad.astype(BF), ((0, 0), (0, -expert_count % 128)))], axis=1
    )
    grad_normed_parts, out_grad, query_grad, side, gains = tail(
        7,
        n_row,
        n_col,
        grad_normed_part.reshape(n_col, tok_rows, model_width),
        out_grad,
        query_grad.astype(BF),
        side,
        gains,
    )
    grad_normed = jnp.sum(grad_normed_parts.astype(F32), axis=0)
    scaled = grad_normed * first_gain
    first_normed = resid_in * first_scale
    grad_first = first_scale * (
        scaled - first_normed * jnp.mean(scaled * first_normed, axis=-1, keepdims=True)
    )
    input_grad = (grad_resid + grad_first).astype(BF)
    query_grad = query_grad.astype(F32)
    out_grad = out_grad.astype(F32)
    kv_width = KEY_VALUE_HEADS * HEAD_SIZE
    key_weight_grad = side[:, :kv_width].astype(F32)
    value_weight_grad = side[:, kv_width : 2 * kv_width].astype(F32)
    router_grad = side[:, 2 * kv_width : 2 * kv_width + expert_count].astype(F32)
    first_gain_grad, second_gain_grad = gains[0], gains[1]
    query_gain_grad, key_gain_grad = gains[2, :HEAD_SIZE], gains[3, :HEAD_SIZE]
    return (
        block_out,
        input_grad,
        first_gain_grad,
        query_grad,
        key_weight_grad,
        value_weight_grad,
        out_grad,
        query_gain_grad,
        key_gain_grad,
        second_gain_grad,
        router_grad,
        gate_grad[None],
        up_grad[None],
        down_grad[None],
    )


def solution(mesh):
    placed = (
        P(("row", "col"), None),
        P(),
        P(None, "col"),
        P(),
        P(),
        P("col", None),
        P(),
        P(),
        P(),
        P(),
        P(("row", "col"), None, None),
        P(("row", "col"), None, None),
        P(("row", "col"), None, None),
        P("row", None),
        P(("row", "col"), None),
        P(("row", "col"), None),
    )
    return jax.shard_map(
        functools.partial(shards, mesh.shape["row"], mesh.shape["col"]),
        mesh=mesh,
        in_specs=placed,
        out_specs=(
            P(("row", "col"), None),
            P(("row", "col"), None),
            P(),
            P(None, "col"),
            P(),
            P(),
            P("col", None),
            P(),
            P(),
            P(),
            P(),
            P(("row", "col"), None, None),
            P(("row", "col"), None, None),
            P(("row", "col"), None, None),
        ),
        check_vma=False,
    )
```
